8 devices in a mesh: dp: 2 (over y, z), ep: 4 (over x, core).
Axes of the slice: x: 2, y: 2, z: 1, core: 2. Of those that a mesh axis runs over, the one named last changes fastest.
Arguments:
- x: bfloat16 [2, 4, 256, 7168], P('dp', 'ep'), parts along dimension 0
- expert: int32 [2, 4, 256, 2], P('dp', 'ep'), parts along dimension 0
- slot: int32 [2, 4, 256, 2], P('dp', 'ep'), parts along dimension 0
- gate: float32 [2, 4, 256, 2], P('dp', 'ep'), parts along dimension 0
- w_gate: bfloat16 [8, 7168, 4864], P('ep')
- w_up: bfloat16 [8, 7168, 4864], P('ep')
- w_down: bfloat16 [8, 4864, 7168], P('ep')
Outputs:
- y: bfloat16 [2, 4, 256, 7168], P('dp', 'ep'), parts along dimension 0
There are 2 independent parts. The reference program is written for one: setup_inputs(seed, part) draws one part's arguments, and reference() takes and returns one part's arrays. A program takes and returns all parts, laid end to end along the dimension named above; an argument that names none is the same for every part.
All inputs are finite; a program needn't handle non-finite values.
Results may differ from the reference program's by a relative error of at most 0.009.
Values are sent between devices in bfloat16 or wider.
A program may use at most 2 GiB of HBM per device.

```python
import jax
import jax.numpy as jnp

MEMBERS = 4
TOKENS = 256
D = 7168
FF = 4864
TOP = 2
EXPERTS = 8
SLOTS = 5 * TOKENS * TOP // (4 * EXPERTS)


def setup_inputs(seed: int = 0, part: int = 0) -> dict:
    own, k1, k2, k3, k4, k5, k6 = jax.random.split(jax.random.key(seed), 7)
    kx, ke, kl, kg = jax.random.split(jax.random.fold_in(own, part), 4)
    devices = (1, MEMBERS)
    place = jax.random.permutation(kl, jnp.arange(EXPERTS, dtype=jnp.uint32))
    slow = ((EXPERTS + (9 * place) % EXPERTS) << ((9 * place) // EXPERTS)) // EXPERTS
    wait = (jax.random.bits(ke, (*devices, TOKENS, EXPERTS), jnp.uint32) >> 10) * slow
    expert = jnp.argsort(wait, axis=-1)[..., :TOP].astype(jnp.int32)
    chosen = jax.nn.one_hot(expert, EXPERTS, dtype=jnp.int32)
    in_line = jnp.cumsum(chosen.reshape(*devices, TOKENS * TOP, EXPERTS), axis=2) - 1
    slot = jnp.sum(in_line.reshape(chosen.shape) * chosen, axis=-1)

    def one(key, rows, columns):
        return (jax.random.normal(key, (rows, columns), jnp.float32) * rows**-0.5).astype(jnp.bfloat16)

    def weights(key, rows, columns):
        return jax.lax.map(lambda k: one(k, rows, columns), jax.random.split(key, EXPERTS))

    return {
        "x": jax.random.normal(kx, (*devices, TOKENS, D), jnp.float32).astype(jnp.bfloat16),
        "expert": expert,
        "slot": slot,
        "gate": jax.nn.softmax(jax.random.normal(kg, expert.shape, jnp.float32)),
        "w_gate": weights(k1, D, FF),
        "w_up": weights(k2, D, FF),
        "w_down": weights(k3, FF, D),
    }


def einsum(form, a, b):
    return jnp.einsum(form, a.astype(jnp.float32), b.astype(jnp.float32))


def reference(x, expert, slot, gate, w_gate, w_up, w_down):
    to_expert = jax.nn.one_hot(expert, EXPERTS, dtype=jnp.bfloat16)
    to_slot = jax.nn.one_hot(slot, SLOTS, dtype=jnp.bfloat16)
    weighted = to_expert * gate[..., None].astype(jnp.bfloat16)
    dispatch = einsum("abtke,abtkc->abtec", to_expert, to_slot).astype(jnp.bfloat16)
    combine = einsum("abtke,abtkc->abtec", weighted, to_slot).astype(jnp.bfloat16)
    z = einsum("abtec,abtd->aebcd", dispatch, x).astype(jnp.bfloat16)
    h = jax.nn.silu(einsum("aebcd,edf->aebcf", z, w_gate))
    h = (h * einsum("aebcd,edf->aebcf", z, w_up)).astype(jnp.bfloat16)
    out = einsum("aebcf,efd->aebcd", h, w_down).astype(jnp.bfloat16)
    y = einsum("abtec,aebcd->abtd", combine, out)
    return y.astype(jnp.bfloat16)
```

```python
import functools

import jax
import jax.numpy as jnp
from jax import lax
from jax.experimental import pallas as pl
from jax.experimental.pallas import tpu as pltpu
from jax.sharding import PartitionSpec as P

MESH = pl.DeviceIdType.MESH
TOK, D, FF, SLOTS = 256, 7168, 4864, 80
ROWS = 4 * SLOTS
KC = 512
NK = D // KC
NT = FF // 256
NC = 512
NN = D // NC
NS = 4
LAG = 3
RING = 4
RINGX = 5
BF, F32 = jnp.bfloat16, jnp.float32


def kernel(x, u, meta, wg, wu, wd, y, xin,
           acc, wbuf, h, z, xs, oh, ct, mrecv, obuf, send3, send1, sendx, y3r, y1r, yxr, yout,
           wsem, lsem, osem, msend, mrsem, csend, crecv, ssend, srecv, fsend, frecv,
           s3, r3, s1, r1, sx, rx):
    me = lax.axis_index("ep")
    pair = me // 2
    sib = pair * 2 + (1 - lax.rem(me, 2))
    far = (1 - pair) * 2 + lax.rem(me, 2)
    diag = (1 - pair) * 2 + (1 - lax.rem(me, 2))
    peers = (sib, far, diag)

    def remote(src, dst, send, recv, to):
        return pltpu.make_async_remote_copy(
            src_ref=src, dst_ref=dst, send_sem=send, recv_sem=recv, device_id={"ep": to}, device_id_type=MESH)

    def kcols(k):
        return pl.ds(pl.multiple_of(k * KC, KC), KC)

    def w1(k, e, m):
        return pltpu.make_async_copy((wg, wu)[m].at[e, kcols(k), :], wbuf.at[2 * e + m], wsem.at[2 * e + m, 0])

    def w2(j):
        n, e, slot = j // 2, lax.rem(j, 2), lax.rem(j, NS)
        col = pl.multiple_of(n * NC, NC)
        out = []
        for b in range(NT // 2):
            out.append(pltpu.make_async_copy(
                wd.at[e, b * 512:(b + 1) * 512, pl.ds(col, NC)],
                wbuf.at[slot, :, b * 512:(b + 1) * 512], wsem.at[slot, b]))
        for q in range(2):
            out.append(pltpu.make_async_copy(
                wd.at[e, FF - 256:, pl.ds(pl.multiple_of(col + q * 256, 256), 256)],
                wbuf.at[slot, q * 256:(q + 1) * 256, FF - 256:], wsem.at[slot, NT // 2 + q]))
        return out

    for m in range(2):
        w1(0, 0, m).start()

    barrier = pltpu.get_barrier_semaphore()
    for p in peers:
        pl.semaphore_signal(barrier, inc=1, device_id={"ep": p}, device_id_type=MESH)
    pl.semaphore_wait(barrier, 3)

    def cross(k):
        return remote(u.at[:, kcols(k)], xin.at[1, :, kcols(k)], csend.at[k], crecv.at[k], far)

    def side(k):
        return remote(x.at[:, kcols(k)], xin.at[0, :, kcols(k)], ssend.at[k], srecv.at[k], sib)

    def forward(k):
        return remote(xin.at[1, :, kcols(k)], xin.at[2, :, kcols(k)], fsend.at[k], frecv.at[k], sib)

    def metas(i):
        return remote(meta.at[peers[i]], mrecv.at[i], msend.at[i], mrsem.at[i], peers[i])

    def loads(k, slot):
        return [pltpu.make_async_copy(src.at[:, kcols(k)], xs.at[slot, i], lsem.at[slot, i])
                for i, src in enumerate((x, xin.at[0], xin.at[1], xin.at[2]))]

    for i in range(3):
        metas(i).start()
    mine = pltpu.make_async_copy(meta.at[me], mrecv.at[3], lsem.at[0, 0])
    mine.start()

    def start_x(k, _):
        cross(k).start()
        side(k).start()
        return 0
    lax.fori_loop(0, NK, start_x, 0)

    acc[...] = jnp.zeros_like(acc)
    obuf[...] = jnp.zeros_like(obuf)
    mine.wait()
    row = lax.broadcasted_iota(jnp.int32, (SLOTS, TOK), 0).astype(F32)
    for s in range(4):
        if s > 0:
            metas(s - 1).wait_recv()
        src = (s - 1) % 4
        parts = []
        for e in range(2):
            hit = row == mrecv[src, e:e + 1, :]
            oh[s, e * SLOTS:(e + 1) * SLOTS, :] = jnp.where(hit, 1.0, 0.0).astype(BF)
            parts.append(jnp.where(hit, mrecv[src, 2 + e:3 + e, :], 0.0))
        full = jnp.concatenate(parts + [jnp.zeros((256 - 2 * SLOTS, TOK), F32)], axis=0)
        ct[s] = jnp.transpose(full).astype(BF)

    def dot(lhs, rhs):
        return jnp.dot(lhs, rhs, preferred_element_type=F32)

    def select(xslot, zslot):
        for s in range(4):
            got = dot(oh[s], xs[xslot, s]).astype(BF)
            for e in range(2):
                z[zslot, e, s * SLOTS:(s + 1) * SLOTS, :] = got[e * SLOTS:(e + 1) * SLOTS]

    def block(zslot, e):
        for c in range(0, FF, 1280):
            cols = slice(c, min(c + 1280, FF))
            for m in range(2):
                acc[e, m, :, cols] += dot(z[zslot, e], wbuf[2 * e + m, :, cols])

    for k in range(2):
        cross(k).wait_recv()
        forward(k).start()
    side(0).wait_recv()
    forward(0).wait_recv()
    for c in loads(0, 0):
        c.start()
    for c in loads(0, 0):
        c.wait()
    select(0, 0)

    def step(k, _):
        now, later = lax.rem(k, 2), lax.rem(k + 1, 2)

        @pl.when(k + 1 < NK)
        def _():
            side(k + 1).wait_recv()
            forward(k + 1).wait_recv()
            for c in loads(k + 1, later):
                c.start()
        for m in range(2):
            w1(k, 1, m).start()
        for m in range(2):
            w1(k, 0, m).wait()
        block(now, 0)

        @pl.when(k + 1 < NK)
        def _():
            for m in range(2):
                w1(k + 1, 0, m).start()
            for c in loads(k + 1, later):
                c.wait()

        @pl.when(k + 2 < NK)
        def _():
            cross(k + 2).wait_recv()
            forward(k + 2).start()
        for m in range(2):
            w1(k, 1, m).wait()
        block(now, 1)
        select(later, later)
        return 0

    lax.fori_loop(0, NK, step, 0)

    for j in range(NS):
        for c in w2(j):
            c.start()

    def act(i, _):
        e = i // NT
        cols = pl.ds(pl.multiple_of(lax.rem(i, NT) * 256, 256), 256)
        g = acc[e, 0, :, cols]
        h[e, :, cols] = (jax.nn.silu(g) * acc[e, 1, :, cols]).astype(BF)
        return 0
    lax.fori_loop(0, 2 * NT, act, 0)

    def held(which, n):
        return (which, n // 9, slice(0, TOK), pl.ds(pl.multiple_of(lax.rem(n, 9) * NC, NC), NC))

    def ncols(n):
        return pl.ds(pl.multiple_of(n * NC, NC), NC)

    def to3(n):
        b, r = lax.rem(n, 2), lax.rem(n, RING)
        return remote(send3.at[b], y3r.at[r], s3.at[b], r3.at[r], sib)

    def to1(n):
        b, r = lax.rem(n, 2), lax.rem(n, RING)
        return remote(send1.at[b], y1r.at[r], s1.at[b], r1.at[r], sib)

    def tox(n):
        b, r = lax.rem(n, 2), lax.rem(n, RINGX)
        return remote(sendx.at[b], yxr.at[r], sx.at[b], rx.at[r], far)

    def out(n):
        b = lax.rem(n, 2)
        return pltpu.make_async_copy(yout.at[b], y.at[:, ncols(n)], osem.at[b])

    def chip_sum(n):
        b, r = lax.rem(n, 2), lax.rem(n, RING)
        sendx[b] = (acc[held(1, n)] + y3r[r].astype(F32)).astype(BF)

    def assemble(n):
        b, r = lax.rem(n, 2), lax.rem(n, RING)
        yout[b] = (acc[held(0, n)] + y1r[r].astype(F32) + yxr[lax.rem(n, RINGX)].astype(F32)).astype(BF)

    def down(e, slot):
        tail = jnp.concatenate([wbuf[slot, q * 256:(q + 1) * 256, FF - 256:] for q in range(2)], axis=1)
        tiles = [wbuf[slot, :, b * 512:(b + 1) * 512] for b in range(NT // 2)] + [tail]
        got = dot(h[e], jnp.concatenate(tiles, axis=0)).astype(BF)
        for s in range(4):
            obuf[s, e * SLOTS:(e + 1) * SLOTS, :] = got[s * SLOTS:(s + 1) * SLOTS]

    def combine(n):
        b = lax.rem(n, 2)
        send3[b] = dot(ct[3], obuf[3]).astype(BF)
        send1[b] = dot(ct[1], obuf[1]).astype(BF)
        acc[held(1, n)] = dot(ct[2], obuf[2])
        acc[held(0, n)] = dot(ct[0], obuf[0])

    def step(n, _):
        @pl.when(n >= 1)
        def _():
            @pl.when(2 * n + 3 < 2 * NN)
            def _():
                for c in w2(2 * n + 3):
                    c.start()

        @pl.when(n >= LAG)
        def _():
            to1(n - LAG).wait_recv()
            tox(n - LAG).wait_recv()

            @pl.when(n >= LAG + 2)
            def _():
                out(n - LAG - 2).wait()
            assemble(n - LAG)
            out(n - LAG).start()
        for c in w2(2 * n):
            c.wait()
        down(0, lax.rem(2 * n, NS))

        @pl.when(2 * n + 4 < 2 * NN)
        def _():
            for c in w2(2 * n + 4):
                c.start()

        @pl.when(n >= 1)
        def _():
            to3(n - 1).wait_recv()

            @pl.when(n >= 3)
            def _():
                tox(n - 3).wait_send()
            chip_sum(n - 1)
            tox(n - 1).start()

        @pl.when(n >= 2)
        def _():
            to3(n - 2).wait_send()
            to1(n - 2).wait_send()
        for c in w2(2 * n + 1):
            c.wait()
        down(1, lax.rem(2 * n + 1, NS))
        combine(n)
        to3(n).start()
        to1(n).start()
        return 0

    lax.fori_loop(0, NN, step, 0)

    last = NN - 1
    to3(last).wait_recv()
    tox(last - 2).wait_send()
    chip_sum(last)
    tox(last).start()
    for n in range(NN - LAG, NN):
        to1(n).wait_recv()
        tox(n).wait_recv()
        out(n - 2).wait()
        assemble(n)
        out(n).start()
    for n in range(NN - 2, NN):
        out(n).wait()
        tox(n).wait_send()
        to3(n).wait_send()
        to1(n).wait_send()

    def drain(k, _):
        cross(k).wait_send()
        side(k).wait_send()
        forward(k).wait_send()
        return 0
    lax.fori_loop(0, NK, drain, 0)
    for i in range(3):
        metas(i).wait_send()


def layer(x, u, meta, wg, wu, wd):
    hbm, vmem, dma = pl.BlockSpec(memory_space=pl.ANY), pltpu.VMEM, pltpu.SemaphoreType.DMA
    chunk = (TOK, NC)
    return pl.pallas_call(
        kernel,
        out_shape=(jax.ShapeDtypeStruct((TOK, D), BF), jax.ShapeDtypeStruct((3, TOK, D), BF)),
        in_specs=[hbm] * 6,
        out_specs=(hbm, hbm),
        scratch_shapes=[
            vmem((2, 2, ROWS, FF), F32),
            vmem((NS, KC, FF), BF),
            vmem((2, ROWS, FF), BF),
            vmem((2, 2, ROWS, KC), BF),
            vmem((2, 4, TOK, KC), BF),
            vmem((4, 2 * SLOTS, TOK), BF),
            vmem((4, TOK, 256), BF),
            vmem((4, 8, TOK), F32),
            vmem((4, 256, NC), BF),
            vmem((2, *chunk), BF),
            vmem((2, *chunk), BF),
            vmem((2, *chunk), BF),
            vmem((RING, *chunk), BF),
            vmem((RING, *chunk), BF),
            vmem((RINGX, *chunk), BF),
            vmem((2, *chunk), BF),
            dma((NS, NT // 2 + 2)), dma((2, 4)), dma((2,)), dma((3,)), dma((3,)),
            dma((NK,)), dma((NK,)), dma((NK,)), dma((NK,)), dma((NK,)), dma((NK,)),
            dma((2,)), dma((RING,)), dma((2,)), dma((RING,)), dma((2,)), dma((RINGX,)),
        ],
        compiler_params=pltpu.CompilerParams(
            collective_id=0, has_side_effects=True, vmem_limit_bytes=67043328),
        name="moe",
    )(x, u, meta, wg, wu, wd)


def solution(mesh):
    def body(x, expert, slot, gate, wg, wu, wd):
        x = x[0, 0]
        expert, slot, gate = expert[0, 0], slot[0, 0], gate[0, 0].astype(BF).astype(F32)
        experts = 2 * mesh.shape["ep"]
        chosen = (expert.T[None] == jnp.arange(experts)[:, None, None]) & (slot.T[None] < SLOTS)
        pos = jnp.sum(jnp.where(chosen, slot.T[None] + 1, 0), axis=1).astype(F32) - 1.0
        weight = jnp.sum(jnp.where(chosen, gate.T[None], 0.0), axis=1)
        meta = jnp.concatenate(
            [pos.reshape(-1, 2, TOK), weight.reshape(-1, 2, TOK), jnp.zeros((experts // 2, 4, TOK), F32)], axis=1)
        return layer(x, x, meta, wg, wu, wd)[0][None, None]

    tok = P("dp", "ep", None, None)
    ex = P("ep", None, None)
    with jax.sharding.use_abstract_mesh(mesh.abstract_mesh):
        return jax.shard_map(
            body, mesh=mesh, in_specs=(tok, tok, tok, tok, ex, ex, ex), out_specs=tok, check_vma=False)
```

```python
import functools

import jax
import jax.numpy as jnp
from jax import lax
from jax.experimental import pallas as pl
from jax.experimental.pallas import tpu as pltpu
from jax.sharding import PartitionSpec as P

MESH = pl.DeviceIdType.MESH
TOK, D, FF, SLOTS = 256, 7168, 4864, 80
ROWS = 4 * SLOTS
KC = 512
NK = D // KC
NT = FF // 256
NC = 512
NN = D // NC
NS = 4
LAG = 3
RING = 4
RINGX = 5
PACKED = 176
BF, F32 = jnp.bfloat16, jnp.float32


def kernel(rows, x, meta, wg, wu, wd, y, xin,
           acc, wbuf, h, z, xs, oh, ct, mown, pack, mrecv, obuf, send3, send1, sendx, y3r, y1r, yxr, yout, perm,
           wsem, lsem, osem, msend, mrsem, csend, crecv, ssend, srecv, fsend, frecv,
           s3, r3, s1, r1, sx, rx):
    packed = rows < TOK
    me = lax.axis_index("ep")
    pair = me // 2
    sib = pair * 2 + (1 - lax.rem(me, 2))
    far = (1 - pair) * 2 + lax.rem(me, 2)
    diag = (1 - pair) * 2 + (1 - lax.rem(me, 2))
    peers = (sib, far, diag)

    def dot(lhs, rhs):
        return jnp.dot(lhs, rhs, preferred_element_type=F32)

    def remote(src, dst, send, recv, to):
        return pltpu.make_async_remote_copy(
            src_ref=src, dst_ref=dst, send_sem=send, recv_sem=recv, device_id={"ep": to}, device_id_type=MESH)

    def kcols(k):
        return pl.ds(pl.multiple_of(k * KC, KC), KC)

    def w1(k, e, m):
        return pltpu.make_async_copy((wg, wu)[m].at[e, kcols(k), :], wbuf.at[2 * e + m], wsem.at[2 * e + m, 0])

    def w2(j):
        n, e, slot = j // 2, lax.rem(j, 2), lax.rem(j, NS)
        col = pl.multiple_of(n * NC, NC)
        out = []
        for b in range(NT // 2):
            out.append(pltpu.make_async_copy(
                wd.at[e, b * 512:(b + 1) * 512, pl.ds(col, NC)],
                wbuf.at[slot, :, b * 512:(b + 1) * 512], wsem.at[slot, b]))
        for q in range(2):
            out.append(pltpu.make_async_copy(
                wd.at[e, FF - 256:, pl.ds(pl.multiple_of(col + q * 256, 256), 256)],
                wbuf.at[slot, q * 256:(q + 1) * 256, FF - 256:], wsem.at[slot, NT // 2 + q]))
        return out

    def packed_x(k):
        return h.at[k // 9, :rows, pl.ds(pl.multiple_of(lax.rem(k, 9) * KC, KC), KC)]

    def cross(k):
        src = packed_x(k) if packed else x.at[:, kcols(k)]
        return remote(src, xin.at[1, :rows, kcols(k)], csend.at[k], crecv.at[k], far)

    def side(k):
        return remote(x.at[:, kcols(k)], xin.at[0, :, kcols(k)], ssend.at[k], srecv.at[k], sib)

    def forward(k):
        return remote(xin.at[1, :rows, kcols(k)], xin.at[2, :rows, kcols(k)], fsend.at[k], frecv.at[k], sib)

    def metas(i):
        src = pack.at[pl.ds(pl.multiple_of(peers[i] * 8, 8), 8)] if packed and i else meta.at[peers[i]]
        return remote(src, mrecv.at[i], msend.at[i], mrsem.at[i], peers[i])

    def loads(k, slot):
        return [pltpu.make_async_copy(src.at[:r, kcols(k)], xs.at[slot, i, :r], lsem.at[slot, i])
                for i, (src, r) in enumerate(((x, TOK), (xin.at[0], TOK), (xin.at[1], rows), (xin.at[2], rows)))]

    for m in range(2):
        w1(0, 0, m).start()
    mine = pltpu.make_async_copy(meta, mown, lsem.at[0, 0])
    mine.start()
    if packed:
        halves = [pltpu.make_async_copy(x.at[:, c:c + w], wbuf.at[2 + i, :TOK, :w], lsem.at[1, i])
                  for i, (c, w) in enumerate(((0, 9 * KC), (9 * KC, D - 9 * KC)))]
        for c in halves:
            c.start()
    barrier = pltpu.get_barrier_semaphore()
    for p in peers:
        pl.semaphore_signal(barrier, inc=1, device_id={"ep": p}, device_id_type=MESH)
    mine.wait()

    def pack_x(k):
        src = wbuf[2 + k // 9, :TOK, pl.ds(pl.multiple_of(lax.rem(k, 9) * KC, KC), KC)]
        packed_x(k)[...] = dot(perm[0, :rows], src).astype(BF)

    if packed:
        need = jnp.zeros((1, TOK), F32)
        for t in range(2):
            there = mown[(1 - pair) * 2 + t]
            need = jnp.maximum(need, jnp.maximum(there[0:1], there[1:2]))
        need = jnp.where(need > 0.0, 1.0, 0.0)
        r_at = lax.broadcasted_iota(jnp.int32, (TOK, TOK), 0)
        c_at = lax.broadcasted_iota(jnp.int32, (TOK, TOK), 1)
        before = jnp.where(r_at < c_at, 1.0, 0.0).astype(BF)
        rank = dot(jnp.broadcast_to(need, (16, TOK)).astype(BF), before)[0:1]
        rank = jnp.where(need > 0.0, rank, -1.0)
        to_row = jnp.where(r_at.astype(F32) == rank, 1.0, 0.0)
        perm[0] = to_row.astype(BF)
        for c in halves:
            c.wait()
        pack_x(0)
        perm[1] = jnp.transpose(to_row).astype(BF)
        pack[...] = dot(mown[...].reshape(4 * 8, TOK).astype(BF), perm[1])
    pl.semaphore_wait(barrier, 3)
    cross(0).start()
    for i in range(3):
        metas(i).start()
    side(0).start()

    def start_x(k, _):
        if packed:
            @pl.when(k < NK)
            def _():
                pack_x(k)

            @pl.when(k > 1)
            def _():
                cross(k - 1).start()
                side(k - 1).start()
        else:
            cross(k).start()
            side(k).start()
        return 0
    lax.fori_loop(1, NK + 1 if packed else NK, start_x, 0)
    if packed:
        for i in range(2):
            xs[i, 2:, rows:] = jnp.zeros((2, TOK - rows, KC), BF)
        yxr[:, rows:] = jnp.zeros((RINGX, TOK - rows, NC), BF)

    def clear(i, _):
        acc[i // 40, lax.rem(i // 20, 2), pl.ds(pl.multiple_of(lax.rem(i, 20) * 16, 16), 16), :] = jnp.zeros((16, FF), F32)
        return 0
    lax.fori_loop(0, 80, clear, 0)
    obuf[...] = jnp.zeros_like(obuf)
    row = lax.broadcasted_iota(jnp.int32, (SLOTS, TOK), 0).astype(F32) + 1.0
    for s in range(4):
        if s > 0:
            metas(s - 1).wait_recv()
            got = mrecv[s - 1]
        else:
            got = mown[me]
        parts = []
        for e in range(2):
            hit = row == got[e:e + 1]
            oh[s, e * SLOTS:(e + 1) * SLOTS, :] = jnp.where(hit, 1.0, 0.0).astype(BF)
            parts.append(jnp.where(hit, got[2 + e:3 + e], 0.0))
        full = jnp.concatenate(parts + [jnp.zeros((256 - 2 * SLOTS, TOK), F32)], axis=0)
        ct[s] = jnp.transpose(full).astype(BF)

    def select(xslot, zslot):
        for s in range(4):
            got = dot(oh[s], xs[xslot, s]).astype(BF)
            for e in range(2):
                z[zslot, e, s * SLOTS:(s + 1) * SLOTS, :] = got[e * SLOTS:(e + 1) * SLOTS]

    def block(zslot, e, last):
        for c in range(0, FF, 1280):
            cols = slice(c, min(c + 1280, FF))
            g, v = (acc[e, m, :, cols] + dot(z[zslot, e], wbuf[2 * e + m, :, cols]) for m in range(2))
            if last:
                h[e, :, cols] = (jax.nn.silu(g) * v).astype(BF)
            else:
                acc[e, 0, :, cols] = g
                acc[e, 1, :, cols] = v

    cross(0).wait_recv()
    forward(0).start()
    side(0).wait_recv()
    forward(0).wait_recv()
    for c in loads(0, 0):
        c.start()
    for c in loads(0, 0):
        c.wait()
    select(0, 0)

    def arrived(k, slot):
        side(k).wait_recv()
        forward(k).wait_recv()
        for c in loads(k, slot):
            c.start()

    def step(k, _):
        now, later = lax.rem(k, 2), lax.rem(k + 1, 2)
        for m in range(2):
            w1(k, 1, m).start()

        @pl.when(k == 0)
        def _():
            cross(1).wait_recv()
            forward(1).start()

        @pl.when(jnp.logical_and(k > 0, k + 1 < NK))
        def _():
            arrived(k + 1, later)
        for m in range(2):
            w1(k, 0, m).wait()
        block(now, 0, False)

        @pl.when(k == 0)
        def _():
            arrived(1, 1)

        @pl.when(k + 1 < NK)
        def _():
            for m in range(2):
                w1(k + 1, 0, m).start()
            for c in loads(k + 1, later):
                c.wait()

        @pl.when(k + 2 < NK)
        def _():
            cross(k + 2).wait_recv()
            forward(k + 2).start()
        for m in range(2):
            w1(k, 1, m).wait()
        block(now, 1, False)
        select(later, later)
        return 0

    lax.fori_loop(0, NK - 1 if packed else NK, step, 0)
    if packed:
        def sent(k, _):
            cross(k).wait_send()
            return 0
        lax.fori_loop(0, NK, sent, 0)
        for m in range(2):
            w1(NK - 1, 1, m).start()
        for m in range(2):
            w1(NK - 1, 0, m).wait()
        block((NK - 1) % 2, 0, True)
        for j in range(2):
            for c in w2(j):
                c.start()
        for m in range(2):
            w1(NK - 1, 1, m).wait()
        block((NK - 1) % 2, 1, True)

    for j in range(2 if packed else 0, NS):
        for c in w2(j):
            c.start()

    def act(i, _):
        e = i // NT
        cols = pl.ds(pl.multiple_of(lax.rem(i, NT) * 256, 256), 256)
        g = acc[e, 0, :, cols]
        h[e, :, cols] = (jax.nn.silu(g) * acc[e, 1, :, cols]).astype(BF)
        return 0
    if not packed:
        lax.fori_loop(0, 2 * NT, act, 0)

    def held(which, n):
        return (which, n // 9, slice(0, rows if which else TOK), pl.ds(pl.multiple_of(lax.rem(n, 9) * NC, NC), NC))

    def ncols(n):
        return pl.ds(pl.multiple_of(n * NC, NC), NC)

    def to3(n):
        b, r = lax.rem(n, 2), lax.rem(n, RING)
        return remote(send3.at[b], y3r.at[r], s3.at[b], r3.at[r], sib)

    def to1(n):
        b, r = lax.rem(n, 2), lax.rem(n, RING)
        return remote(send1.at[b], y1r.at[r], s1.at[b], r1.at[r], sib)

    def tox(n):
        b, r = lax.rem(n, 2), lax.rem(n, RINGX)
        return remote(sendx.at[b], yxr.at[r, :rows], sx.at[b], rx.at[r], far)

    def out(n):
        b = lax.rem(n, 2)
        return pltpu.make_async_copy(yout.at[b], y.at[:, ncols(n)], osem.at[b])

    def chip_sum(n):
        b, r = lax.rem(n, 2), lax.rem(n, RING)
        sendx[b] = (acc[held(1, n)] + y3r[r].astype(F32)).astype(BF)

    def assemble(n):
        b, r = lax.rem(n, 2), lax.rem(n, RING)
        cross_part = yxr[lax.rem(n, RINGX)]
        cross_part = dot(perm[1], cross_part) if packed else cross_part.astype(F32)
        yout[b] = (acc[held(0, n)] + y1r[r].astype(F32) + cross_part).astype(BF)

    def down(e, slot):
        tail = jnp.concatenate([wbuf[slot, q * 256:(q + 1) * 256, FF - 256:] for q in range(2)], axis=1)
        tiles = [wbuf[slot, :, b * 512:(b + 1) * 512] for b in range(NT // 2)] + [tail]
        got = dot(h[e], jnp.concatenate(tiles, axis=0)).astype(BF)
        for s in range(4):
            obuf[s, e * SLOTS:(e + 1) * SLOTS, :] = got[s * SLOTS:(s + 1) * SLOTS]

    def combine(n):
        b = lax.rem(n, 2)
        send3[b] = dot(ct[3, :rows], obuf[3]).astype(BF)
        send1[b] = dot(ct[1], obuf[1]).astype(BF)
        acc[held(1, n)] = dot(ct[2, :rows], obuf[2])
        acc[held(0, n)] = dot(ct[0], obuf[0])

    def step(n, _):
        @pl.when(n >= 1)
        def _():
            @pl.when(2 * n + 3 < 2 * NN)
            def _():
                for c in w2(2 * n + 3):
                    c.start()

        @pl.when(n >= LAG)
        def _():
            to1(n - LAG).wait_recv()
            tox(n - LAG).wait_recv()

            @pl.when(n >= LAG + 2)
            def _():
                out(n - LAG - 2).wait()
            assemble(n - LAG)
            out(n - LAG).start()
        for c in w2(2 * n):
            c.wait()
        down(0, lax.rem(2 * n, NS))

        @pl.when(2 * n + 4 < 2 * NN)
        def _():
            for c in w2(2 * n + 4):
                c.start()

        @pl.when(n >= 1)
        def _():
            to3(n - 1).wait_recv()

            @pl.when(n >= 3)
            def _():
                tox(n - 3).wait_send()
            chip_sum(n - 1)
            tox(n - 1).start()

        @pl.when(n >= 2)
        def _():
            to3(n - 2).wait_send()
            to1(n - 2).wait_send()
        for c in w2(2 * n + 1):
            c.wait()
        down(1, lax.rem(2 * n + 1, NS))
        combine(n)
        to3(n).start()
        to1(n).start()
        return 0

    lax.fori_loop(0, NN, step, 0)

    last = NN - 1
    to3(last).wait_recv()
    tox(last - 2).wait_send()
    chip_sum(last)
    tox(last).start()
    for n in range(NN - LAG, NN):
        to1(n).wait_recv()
        tox(n).wait_recv()
        out(n - 2).wait()
        assemble(n)
        out(n).start()
    for n in range(NN - 2, NN):
        out(n).wait()
        tox(n).wait_send()
        to3(n).wait_send()
        to1(n).wait_send()

    def drain(k, _):
        if not packed:
            cross(k).wait_send()
        side(k).wait_send()
        forward(k).wait_send()
        return 0
    lax.fori_loop(0, NK, drain, 0)
    for i in range(3):
        metas(i).wait_send()


def route(expert, slot, gate, meta, most, mine, got, ssem, rsem):
    dp, ep = lax.axis_index("dp"), lax.axis_index("ep")
    ep_of = (ep, (ep // 2) * 2 + (1 - lax.rem(ep, 2)), lax.rem(ep + 2, 4), ((ep // 2) * 2 + (1 - lax.rem(ep, 2)) + 2) % 4)
    peers = [(lax.rem(dp + i // 4, 2), ep_of[i % 4]) for i in range(1, 8)]
    barrier = pltpu.get_barrier_semaphore()
    for a, b in peers:
        pl.semaphore_signal(barrier, inc=1, device_id={"dp": a, "ep": b}, device_id_type=MESH)
    which = lax.broadcasted_iota(jnp.int32, (8, TOK), 0)
    place, weight = jnp.zeros((8, TOK), F32), jnp.zeros((8, TOK), F32)
    for j in range(2):
        s = slot[j:j + 1, :]
        hit = (expert[j:j + 1, :] == which) & (s < SLOTS)
        place = jnp.where(hit, (s + 1).astype(F32), place)
        weight = jnp.where(hit, gate[j:j + 1, :].astype(BF).astype(F32), weight)
    away = jnp.max(jnp.where(which // 4 != ep // 2, place, 0.0), axis=0, keepdims=True)
    count = jnp.sum(jnp.where(away > 0.0, 1.0, 0.0), axis=1, keepdims=True)
    mine[...] = jnp.broadcast_to(count, mine.shape)
    for p in range(4):
        meta[p, 0:2] = place[2 * p:2 * p + 2]
        meta[p, 2:4] = weight[2 * p:2 * p + 2]
        meta[p, 4:8] = jnp.zeros((4, TOK), F32)
    copies = [pltpu.make_async_remote_copy(
        src_ref=mine, dst_ref=got.at[i], send_sem=ssem.at[i], recv_sem=rsem.at[i],
        device_id={"dp": a, "ep": b}, device_id_type=MESH) for i, (a, b) in enumerate(peers)]
    pl.semaphore_wait(barrier, 7)
    for c in copies:
        c.start()
    top = mine[...]
    for i, c in enumerate(copies):
        c.wait_recv()
        top = jnp.maximum(top, got[i])
    most[...] = top
    for c in copies:
        c.wait_send()


def routing(expert, slot, gate):
    vmem, dma = pltpu.VMEM, pltpu.SemaphoreType.DMA
    return pl.pallas_call(
        route,
        out_shape=(jax.ShapeDtypeStruct((4, 8, TOK), F32), jax.ShapeDtypeStruct((8, 128), F32)),
        in_specs=[pl.BlockSpec(memory_space=vmem)] * 3,
        out_specs=(pl.BlockSpec(memory_space=vmem),) * 2,
        scratch_shapes=[vmem((8, 128), F32), vmem((7, 8, 128), F32), dma((7,)), dma((7,))],
        compiler_params=pltpu.CompilerParams(collective_id=2, has_side_effects=True),
        name="route",
    )(expert, slot, gate)


def layer(rows, x, meta, wg, wu, wd):
    hbm, vmem, dma = pl.BlockSpec(memory_space=pl.ANY), pltpu.VMEM, pltpu.SemaphoreType.DMA
    chunk, part = (TOK, NC), (rows, NC)
    return pl.pallas_call(
        functools.partial(kernel, rows),
        out_shape=(jax.ShapeDtypeStruct((TOK, D), BF), jax.ShapeDtypeStruct((3, TOK, D), BF)),
        in_specs=[hbm] * 5,
        out_specs=(hbm, hbm),
        scratch_shapes=[
            vmem((2, 2, ROWS, FF), F32),
            vmem((NS, KC, FF), BF),
            vmem((2, ROWS, FF), BF),
            vmem((2, 2, ROWS, KC), BF),
            vmem((2, 4, TOK, KC), BF),
            vmem((4, 2 * SLOTS, TOK), BF),
            vmem((4, TOK, 256), BF),
            vmem((4, 8, TOK), F32),
            vmem((32, TOK), F32),
            vmem((3, 8, TOK), F32),
            vmem((4, 256, NC), BF),
            vmem((2, *part), BF),
            vmem((2, *chunk), BF),
            vmem((2, *part), BF),
            vmem((RING, *part), BF),
            vmem((RING, *chunk), BF),
            vmem((RINGX, *chunk), BF),
            vmem((2, *chunk), BF),
            vmem((2, TOK, TOK), BF),
            dma((NS, NT // 2 + 2)), dma((2, 4)), dma((2,)), dma((3,)), dma((3,)),
            dma((NK,)), dma((NK,)), dma((NK,)), dma((NK,)), dma((NK,)), dma((NK,)),
            dma((2,)), dma((RING,)), dma((2,)), dma((RING,)), dma((2,)), dma((RINGX,)),
        ],
        compiler_params=pltpu.CompilerParams(
            collective_id=int(rows < TOK), has_side_effects=True, vmem_limit_bytes=67043328),
        name=f"moe_{rows}",
    )(x, meta, wg, wu, wd)[0]


def solution(mesh):
    def body(x, expert, slot, gate, wg, wu, wd):
        x = x[0, 0]
        meta, most = routing(expert[0, 0].T, slot[0, 0].T, gate[0, 0].T)
        y = lax.cond(most[0, 0] <= PACKED, functools.partial(layer, PACKED), functools.partial(layer, TOK),
                     x, meta, wg, wu, wd)
        return y[None, None]

    tok = P("dp", "ep", None, None)
    ex = P("ep", None, None)
    with jax.sharding.use_abstract_mesh(mesh.abstract_mesh):
        return jax.shard_map(
            body, mesh=mesh, in_specs=(tok, tok, tok, tok, ex, ex, ex), out_specs=tok, check_vma=False)
```

```python
import functools

import jax
import jax.numpy as jnp
from jax import lax
from jax.experimental import pallas as pl
from jax.experimental.pallas import tpu as pltpu
from jax.sharding import PartitionSpec as P

MESH = pl.DeviceIdType.MESH
TOK, D, FF, SLOTS = 256, 7168, 4864, 80
ROWS = 4 * SLOTS
KC = 512
NK = D // KC
NT = FF // 256
NC = 512
NN = D // NC
NS = 4
LAG = 3
RING = 4
RINGX = 5
PACKED = 160
BF, F32 = jnp.bfloat16, jnp.float32


def kernel(rows, x, meta, wg, wu, wd, y, xin,
           acc, wbuf, h, z, xs, oh, ct, mown, pack, mrecv, obuf, send3, send1, sendx, y3r, y1r, yxr, yout, perm,
           wsem, lsem, osem, msend, mrsem, csend, crecv, ssend, srecv, fsend, frecv,
           s3, r3, s1, r1, sx, rx):
    packed = rows < TOK
    me = lax.axis_index("ep")
    pair = me // 2
    sib = pair * 2 + (1 - lax.rem(me, 2))
    far = (1 - pair) * 2 + lax.rem(me, 2)
    diag = (1 - pair) * 2 + (1 - lax.rem(me, 2))
    peers = (sib, far, diag)

    def dot(lhs, rhs):
        return jnp.dot(lhs, rhs, preferred_element_type=F32)

    def remote(src, dst, send, recv, to):
        return pltpu.make_async_remote_copy(
            src_ref=src, dst_ref=dst, send_sem=send, recv_sem=recv, device_id={"ep": to}, device_id_type=MESH)

    def kcols(k):
        return pl.ds(pl.multiple_of(k * KC, KC), KC)

    def w1(k, e, m):
        return pltpu.make_async_copy((wg, wu)[m].at[e, kcols(k), :], wbuf.at[2 * e + m], wsem.at[2 * e + m, 0])

    def w2(j):
        n, e, slot = j // 2, lax.rem(j, 2), lax.rem(j, NS)
        col = pl.multiple_of(n * NC, NC)
        out = []
        for b in range(NT // 2):
            out.append(pltpu.make_async_copy(
                wd.at[e, b * 512:(b + 1) * 512, pl.ds(col, NC)],
                wbuf.at[slot, :, b * 512:(b + 1) * 512], wsem.at[slot, b]))
        for q in range(2):
            out.append(pltpu.make_async_copy(
                wd.at[e, FF - 256:, pl.ds(pl.multiple_of(col + q * 256, 256), 256)],
                wbuf.at[slot, q * 256:(q + 1) * 256, FF - 256:], wsem.at[slot, NT // 2 + q]))
        return out

    def packed_x(k):
        return h.at[k // 9, :rows, pl.ds(pl.multiple_of(lax.rem(k, 9) * KC, KC), KC)]

    def cross(k):
        src = packed_x(k) if packed else x.at[:, kcols(k)]
        return remote(src, xin.at[1, :rows, kcols(k)], csend.at[k], crecv.at[k], far)

    def side(k):
        return remote(x.at[:, kcols(k)], xin.at[0, :, kcols(k)], ssend.at[k], srecv.at[k], sib)

    def forward(k):
        return remote(xin.at[1, :rows, kcols(k)], xin.at[2, :rows, kcols(k)], fsend.at[k], frecv.at[k], sib)

    def metas(i):
        src = pack.at[pl.ds(pl.multiple_of(peers[i] * 8, 8), 8)] if packed and i else meta.at[peers[i]]
        return remote(src, mrecv.at[i], msend.at[i], mrsem.at[i], peers[i])

    def loads(k, slot):
        return [pltpu.make_async_copy(src.at[:r, kcols(k)], xs.at[slot, i, :r], lsem.at[slot, i])
                for i, (src, r) in enumerate(((x, TOK), (xin.at[0], TOK), (xin.at[1], rows), (xin.at[2], rows)))]

    for m in range(2):
        w1(0, 0, m).start()
    mine = pltpu.make_async_copy(meta, mown, lsem.at[0, 0])
    mine.start()
    if packed:
        halves = [pltpu.make_async_copy(x.at[:, c:c + w], wbuf.at[2 + i, :TOK, :w], lsem.at[1, i])
                  for i, (c, w) in enumerate(((0, 9 * KC), (9 * KC, D - 9 * KC)))]
        for c in halves:
            c.start()
    barrier = pltpu.get_barrier_semaphore()
    for p in peers:
        pl.semaphore_signal(barrier, inc=1, device_id={"ep": p}, device_id_type=MESH)
    mine.wait()

    def pack_x(k):
        src = wbuf[2 + k // 9, :TOK, pl.ds(pl.multiple_of(lax.rem(k, 9) * KC, KC), KC)]
        packed_x(k)[...] = dot(perm[0, :rows], src).astype(BF)

    if packed:
        need = jnp.zeros((1, TOK), F32)
        for t in range(2):
            there = mown[(1 - pair) * 2 + t]
            need = jnp.maximum(need, jnp.maximum(there[0:1], there[1:2]))
        need = jnp.where(need > 0.0, 1.0, 0.0)
        r_at = lax.broadcasted_iota(jnp.int32, (TOK, TOK), 0)
        c_at = lax.broadcasted_iota(jnp.int32, (TOK, TOK), 1)
        before = jnp.where(r_at < c_at, 1.0, 0.0).astype(BF)
        rank = dot(jnp.broadcast_to(need, (16, TOK)).astype(BF), before)[0:1]
        rank = jnp.where(need > 0.0, rank, -1.0)
        to_row = jnp.where(r_at.astype(F32) == rank, 1.0, 0.0)
        perm[0] = to_row.astype(BF)
        for c in halves:
            c.wait()
        pack_x(0)
        perm[1] = jnp.transpose(to_row).astype(BF)
        pack[...] = dot(mown[...].reshape(4 * 8, TOK).astype(BF), perm[1])
    pl.semaphore_wait(barrier, 3)
    cross(0).start()
    for i in range(3):
        metas(i).start()
    side(0).start()

    def start_x(k, _):
        if packed:
            @pl.when(k < NK)
            def _():
                pack_x(k)

            @pl.when(k > 1)
            def _():
                cross(k - 1).start()
                side(k - 1).start()
        else:
            cross(k).start()
            side(k).start()
        return 0
    lax.fori_loop(1, NK + 1 if packed else NK, start_x, 0)
    if packed:
        for i in range(2):
            xs[i, 2:, rows:] = jnp.zeros((2, TOK - rows, KC), BF)
        yxr[:, rows:] = jnp.zeros((RINGX, TOK - rows, NC), BF)

    def clear(i, _):
        acc[i // 40, lax.rem(i // 20, 2), pl.ds(pl.multiple_of(lax.rem(i, 20) * 16, 16), 16), :] = jnp.zeros((16, FF), F32)
        return 0
    lax.fori_loop(0, 80, clear, 0)
    obuf[...] = jnp.zeros_like(obuf)
    row = lax.broadcasted_iota(jnp.int32, (SLOTS, TOK), 0).astype(F32) + 1.0
    for s in range(4):
        if s > 0:
            metas(s - 1).wait_recv()
            got = mrecv[s - 1]
        else:
            got = mown[me]
        parts = []
        for e in range(2):
            hit = row == got[e:e + 1]
            oh[s, e * SLOTS:(e + 1) * SLOTS, :] = jnp.where(hit, 1.0, 0.0).astype(BF)
            parts.append(jnp.where(hit, got[2 + e:3 + e], 0.0))
        full = jnp.concatenate(parts + [jnp.zeros((256 - 2 * SLOTS, TOK), F32)], axis=0)
        ct[s] = jnp.transpose(full).astype(BF)

    def select(xslot, zslot):
        for s in range(4):
            got = dot(oh[s], xs[xslot, s]).astype(BF)
            for e in range(2):
                z[zslot, e, s * SLOTS:(s + 1) * SLOTS, :] = got[e * SLOTS:(e + 1) * SLOTS]

    def block(zslot, e, last):
        for c in range(0, FF, 1280):
            cols = slice(c, min(c + 1280, FF))
            g, v = (acc[e, m, :, cols] + dot(z[zslot, e], wbuf[2 * e + m, :, cols]) for m in range(2))
            if last:
                h[e, :, cols] = (jax.nn.silu(g) * v).astype(BF)
            else:
                acc[e, 0, :, cols] = g
                acc[e, 1, :, cols] = v

    cross(0).wait_recv()
    forward(0).start()
    side(0).wait_recv()
    forward(0).wait_recv()
    for c in loads(0, 0):
        c.start()
    for c in loads(0, 0):
        c.wait()
    select(0, 0)

    def arrived(k, slot):
        side(k).wait_recv()
        forward(k).wait_recv()
        for c in loads(k, slot):
            c.start()

    def step(k, _):
        now, later = lax.rem(k, 2), lax.rem(k + 1, 2)
        for m in range(2):
            w1(k, 1, m).start()

        @pl.when(k == 0)
        def _():
            cross(1).wait_recv()
            forward(1).start()

        @pl.when(jnp.logical_and(k > 0, k + 1 < NK))
        def _():
            arrived(k + 1, later)
        for m in range(2):
            w1(k, 0, m).wait()
        block(now, 0, False)

        @pl.when(k == 0)
        def _():
            arrived(1, 1)

        @pl.when(k + 1 < NK)
        def _():
            for m in range(2):
                w1(k + 1, 0, m).start()
            for c in loads(k + 1, later):
                c.wait()

        @pl.when(k + 2 < NK)
        def _():
            cross(k + 2).wait_recv()
            forward(k + 2).start()
        for m in range(2):
            w1(k, 1, m).wait()
        block(now, 1, False)
        select(later, later)
        return 0

    lax.fori_loop(0, NK - 1 if packed else NK, step, 0)
    if packed:
        def sent(k, _):
            cross(k).wait_send()
            return 0
        lax.fori_loop(0, NK, sent, 0)
        for m in range(2):
            w1(NK - 1, 1, m).start()
        for m in range(2):
            w1(NK - 1, 0, m).wait()
        block((NK - 1) % 2, 0, True)
        for j in range(2):
            for c in w2(j):
                c.start()
        for m in range(2):
            w1(NK - 1, 1, m).wait()
        block((NK - 1) % 2, 1, True)

    for j in range(2 if packed else 0, NS):
        for c in w2(j):
            c.start()

    def act(i, _):
        e = i // NT
        cols = pl.ds(pl.multiple_of(lax.rem(i, NT) * 256, 256), 256)
        g = acc[e, 0, :, cols]
        h[e, :, cols] = (jax.nn.silu(g) * acc[e, 1, :, cols]).astype(BF)
        return 0
    if not packed:
        lax.fori_loop(0, 2 * NT, act, 0)

    def held(which, n):
        return (which, n // 9, slice(0, rows if which else TOK), pl.ds(pl.multiple_of(lax.rem(n, 9) * NC, NC), NC))

    def ncols(n):
        return pl.ds(pl.multiple_of(n * NC, NC), NC)

    def to3(n):
        b, r = lax.rem(n, 2), lax.rem(n, RING)
        return remote(send3.at[b], y3r.at[r], s3.at[b], r3.at[r], sib)

    def to1(n):
        b, r = lax.rem(n, 2), lax.rem(n, RING)
        return remote(send1.at[b], y1r.at[r], s1.at[b], r1.at[r], sib)

    def tox(n):
        b, r = lax.rem(n, 2), lax.rem(n, RINGX)
        return remote(sendx.at[b], yxr.at[r, :rows], sx.at[b], rx.at[r], far)

    def out(n):
        b = lax.rem(n, 2)
        return pltpu.make_async_copy(yout.at[b], y.at[:, ncols(n)], osem.at[b])

    def chip_sum(n):
        b, r = lax.rem(n, 2), lax.rem(n, RING)
        sendx[b] = (acc[held(1, n)] + y3r[r].astype(F32)).astype(BF)

    def assemble(n):
        b, r = lax.rem(n, 2), lax.rem(n, RING)
        cross_part = yxr[lax.rem(n, RINGX)]
        cross_part = dot(perm[1], cross_part) if packed else cross_part.astype(F32)
        yout[b] = (acc[held(0, n)] + y1r[r].astype(F32) + cross_part).astype(BF)

    def down(e, slot):
        tail = jnp.concatenate([wbuf[slot, q * 256:(q + 1) * 256, FF - 256:] for q in range(2)], axis=1)
        tiles = [wbuf[slot, :, b * 512:(b + 1) * 512] for b in range(NT // 2)] + [tail]
        got = dot(h[e], jnp.concatenate(tiles, axis=0)).astype(BF)
        for s in range(4):
            obuf[s, e * SLOTS:(e + 1) * SLOTS, :] = got[s * SLOTS:(s + 1) * SLOTS]

    def combine(n):
        b = lax.rem(n, 2)
        send3[b] = dot(ct[3, :rows], obuf[3]).astype(BF)
        send1[b] = dot(ct[1], obuf[1]).astype(BF)
        acc[held(1, n)] = dot(ct[2, :rows], obuf[2])
        acc[held(0, n)] = dot(ct[0], obuf[0])

    def step(n, _):
        @pl.when(n >= 1)
        def _():
            @pl.when(2 * n + 3 < 2 * NN)
            def _():
                for c in w2(2 * n + 3):
                    c.start()

        @pl.when(n >= LAG)
        def _():
            to1(n - LAG).wait_recv()
            tox(n - LAG).wait_recv()

            @pl.when(n >= LAG + 2)
            def _():
                out(n - LAG - 2).wait()
            assemble(n - LAG)
            out(n - LAG).start()
        for c in w2(2 * n):
            c.wait()
        down(0, lax.rem(2 * n, NS))

        @pl.when(2 * n + 4 < 2 * NN)
        def _():
            for c in w2(2 * n + 4):
                c.start()

        @pl.when(n >= 1)
        def _():
            to3(n - 1).wait_recv()

            @pl.when(n >= 3)
            def _():
                tox(n - 3).wait_send()
            chip_sum(n - 1)
            tox(n - 1).start()

        @pl.when(n >= 2)
        def _():
            to3(n - 2).wait_send()
            to1(n - 2).wait_send()
        for c in w2(2 * n + 1):
            c.wait()
        down(1, lax.rem(2 * n + 1, NS))
        combine(n)
        to3(n).start()
        to1(n).start()
        return 0

    lax.fori_loop(0, NN, step, 0)

    last = NN - 1
    to3(last).wait_recv()
    tox(last - 2).wait_send()
    chip_sum(last)
    tox(last).start()
    for n in range(NN - LAG, NN):
        to1(n).wait_recv()
        tox(n).wait_recv()
        out(n - 2).wait()
        assemble(n)
        out(n).start()
    for n in range(NN - 2, NN):
        out(n).wait()
        tox(n).wait_send()
        to3(n).wait_send()
        to1(n).wait_send()

    def drain(k, _):
        if not packed:
            cross(k).wait_send()
        side(k).wait_send()
        forward(k).wait_send()
        return 0
    lax.fori_loop(0, NK, drain, 0)
    for i in range(3):
        metas(i).wait_send()


def route(expert, slot, gate, meta, most, mine, got, ssem, rsem):
    dp, ep = lax.axis_index("dp"), lax.axis_index("ep")
    ep_of = (ep, (ep // 2) * 2 + (1 - lax.rem(ep, 2)), lax.rem(ep + 2, 4), ((ep // 2) * 2 + (1 - lax.rem(ep, 2)) + 2) % 4)
    peers = [(lax.rem(dp + i // 4, 2), ep_of[i % 4]) for i in range(1, 8)]
    barrier = pltpu.get_barrier_semaphore()
    for a, b in peers:
        pl.semaphore_signal(barrier, inc=1, device_id={"dp": a, "ep": b}, device_id_type=MESH)
    which = lax.broadcasted_iota(jnp.int32, (8, TOK), 0)
    place, weight = jnp.zeros((8, TOK), F32), jnp.zeros((8, TOK), F32)
    for j in range(2):
        s = slot[j:j + 1, :]
        hit = (expert[j:j + 1, :] == which) & (s < SLOTS)
        place = jnp.where(hit, (s + 1).astype(F32), place)
        weight = jnp.where(hit, gate[j:j + 1, :].astype(BF).astype(F32), weight)
    away = jnp.max(jnp.where(which // 4 != ep // 2, place, 0.0), axis=0, keepdims=True)
    count = jnp.sum(jnp.where(away > 0.0, 1.0, 0.0), axis=1, keepdims=True)
    mine[...] = jnp.broadcast_to(count, mine.shape)
    for p in range(4):
        meta[p, 0:2] = place[2 * p:2 * p + 2]
        meta[p, 2:4] = weight[2 * p:2 * p + 2]
        meta[p, 4:8] = jnp.zeros((4, TOK), F32)
    copies = [pltpu.make_async_remote_copy(
        src_ref=mine, dst_ref=got.at[i], send_sem=ssem.at[i], recv_sem=rsem.at[i],
        device_id={"dp": a, "ep": b}, device_id_type=MESH) for i, (a, b) in enumerate(peers)]
    pl.semaphore_wait(barrier, 7)
    for c in copies:
        c.start()
    top = mine[...]
    for i, c in enumerate(copies):
        c.wait_recv()
        top = jnp.maximum(top, got[i])
    most[...] = top
    for c in copies:
        c.wait_send()


def routing(expert, slot, gate):
    vmem, dma = pltpu.VMEM, pltpu.SemaphoreType.DMA
    return pl.pallas_call(
        route,
        out_shape=(jax.ShapeDtypeStruct((4, 8, TOK), F32), jax.ShapeDtypeStruct((8, 128), F32)),
        in_specs=[pl.BlockSpec(memory_space=vmem)] * 3,
        out_specs=(pl.BlockSpec(memory_space=vmem),) * 2,
        scratch_shapes=[vmem((8, 128), F32), vmem((7, 8, 128), F32), dma((7,)), dma((7,))],
        compiler_params=pltpu.CompilerParams(collective_id=2, has_side_effects=True),
        name="route",
    )(expert, slot, gate)


def layer(rows, x, meta, wg, wu, wd):
    hbm, vmem, dma = pl.BlockSpec(memory_space=pl.ANY), pltpu.VMEM, pltpu.SemaphoreType.DMA
    chunk, part = (TOK, NC), (rows, NC)
    return pl.pallas_call(
        functools.partial(kernel, rows),
        out_shape=(jax.ShapeDtypeStruct((TOK, D), BF), jax.ShapeDtypeStruct((3, TOK, D), BF)),
        in_specs=[hbm] * 5,
        out_specs=(hbm, hbm),
        scratch_shapes=[
            vmem((2, 2, ROWS, FF), F32),
            vmem((NS, KC, FF), BF),
            vmem((2, ROWS, FF), BF),
            vmem((2, 2, ROWS, KC), BF),
            vmem((2, 4, TOK, KC), BF),
            vmem((4, 2 * SLOTS, TOK), BF),
            vmem((4, TOK, 256), BF),
            vmem((4, 8, TOK), F32),
            vmem((32, TOK), F32),
            vmem((3, 8, TOK), F32),
            vmem((4, 256, NC), BF),
            vmem((2, *part), BF),
            vmem((2, *chunk), BF),
            vmem((2, *part), BF),
            vmem((RING, *part), BF),
            vmem((RING, *chunk), BF),
            vmem((RINGX, *chunk), BF),
            vmem((2, *chunk), BF),
            vmem((2, TOK, TOK), BF),
            dma((NS, NT // 2 + 2)), dma((2, 4)), dma((2,)), dma((3,)), dma((3,)),
            dma((NK,)), dma((NK,)), dma((NK,)), dma((NK,)), dma((NK,)), dma((NK,)),
            dma((2,)), dma((RING,)), dma((2,)), dma((RING,)), dma((2,)), dma((RINGX,)),
        ],
        compiler_params=pltpu.CompilerParams(
            collective_id=int(rows < TOK), has_side_effects=True, vmem_limit_bytes=67043328),
        name=f"moe_{rows}",
    )(x, meta, wg, wu, wd)[0]


def solution(mesh):
    def body(x, expert, slot, gate, wg, wu, wd):
        x = x[0, 0]
        meta, most = routing(expert[0, 0].T, slot[0, 0].T, gate[0, 0].T)
        y = lax.cond(most[0, 0] <= PACKED, functools.partial(layer, PACKED), functools.partial(layer, TOK),
                     x, meta, wg, wu, wd)
        return y[None, None]

    tok = P("dp", "ep", None, None)
    ex = P("ep", None, None)
    with jax.sharding.use_abstract_mesh(mesh.abstract_mesh):
        return jax.shard_map(
            body, mesh=mesh, in_specs=(tok, tok, tok, tok, ex, ex, ex), out_specs=tok, check_vma=False)
```
